32 devices in a mesh: outer: 4 (over y, core), inner: 8 (over z, x).
Axes of the slice: x: 2, y: 2, z: 4, core: 2. Of those that a mesh axis runs over, the one named last changes fastest.
Arguments:
- queries: bfloat16 [4096, 4096], P(('outer', 'inner')), may hold values from -40 to 40
- keys: bfloat16 [4096, 512], P(('outer', 'inner')), may hold values from -4 to 4
- values: bfloat16 [4096, 512], P(('outer', 'inner')), may hold values from -6 to 6
- doc_lengths: int32 [16], replicated, may hold values from 1 to 1024, 4096 in all
Outputs:
- attended: bfloat16 [4096, 4096], P(('outer', 'inner'))
The draws below stay inside these ranges and needn't reach their ends.
All inputs are finite; a program needn't handle non-finite values.
Results may differ from the reference program's by a relative error of at most 0.005.
Values may be sent and summed in bfloat16 or wider, within the bound.
No kernel may reach another device: no remote copies, remote signals or barrier semaphores. Data moves between devices by JAX's collectives and lax.ppermute only.
A program may use at most 256 MiB of HBM per device.

```python
import math
import jax
import jax.numpy as jnp
import numpy as np
from jax import lax

HEADS = 32
GROUPS = 4
HEAD_DIM = 128
TOK_DEV = 128
DOCS = 16
OUTER_STEPS = 2
SEQ = 4096
N_INNER = 8


def common_draw(key):
    base_key = jax.random.fold_in(key, 7)
    keys = jnp.clip(jax.random.normal(jax.random.fold_in(base_key, 1), (SEQ, GROUPS * HEAD_DIM), jnp.float32), -4.0, 4.0)
    queries = jnp.clip(jax.random.normal(jax.random.fold_in(base_key, 2), (SEQ, HEADS * HEAD_DIM), jnp.float32), -4.0, 4.0)
    return (queries, keys)


def draw_queries(key, part):
    return common_draw(key)[0].astype(jnp.bfloat16)


def draw_keys(key, part):
    return common_draw(key)[1].astype(jnp.bfloat16)


def steps_of(own_key, extent, cuts, low, largest):
    factor_of, own = 1.0, jax.random.fold_in(own_key, 6)
    for dim, shards_of in cuts:
        draws = jnp.exp(jax.random.uniform(jax.random.fold_in(own, dim), (shards_of,), jnp.float32, low / len(cuts), largest / len(cuts)))
        factor_of = factor_of * jnp.repeat(draws, extent[dim] // shards_of).reshape([-1 if axis == dim else 1 for axis in range(len(extent))])
    return factor_of


def length_profile(number_of, total, most, lean):
    loads = [(1 << 20) // math.isqrt(grade ** lean) + 1 for grade in range(2, number_of + 1)]
    surplus, counts = total - most - (number_of - 1), [1] * (number_of - 1)
    while surplus > 0:
        candidates = [i for i in range(number_of - 1) if counts[i] < most]
        pool, budget = sum([loads[i] for i in candidates]), surplus
        for i in candidates:
            more = min(most - counts[i], max(1, budget * loads[i] // pool), surplus)
            counts[i] = counts[i] + more
            surplus = surplus - more
    return np.array([most] + counts)


def ragged(key, amount, total, bound, lean):
    if amount == 2:
        one = jax.random.randint(key, (), max(1, total - bound), min(bound, total - 1) + 1)
        return jnp.stack([one, total - one])
    sizes = jnp.asarray(length_profile(amount, total, bound, lean), jnp.int32)
    couples = (amount - 1) // 2
    source_of, receiver = sizes[1:1 + 2 * couples:2], sizes[2:2 + 2 * couples:2]
    slack = jnp.minimum(source_of - 1, bound - receiver)
    moved = jax.random.randint(jax.random.fold_in(key, 1), (couples,), 0, 1 << 20) % (slack + 1)
    sizes = sizes.at[1:1 + 2 * couples:2].set(source_of - moved).at[2:2 + 2 * couples:2].set(receiver + moved)
    return sizes[jax.random.permutation(jax.random.fold_in(key, 2), amount)]


def bell_draw(stream_key, dims, deviation, most, pieces=(), kind=jnp.bfloat16):
    entries = deviation * jax.random.normal(stream_key, dims, jnp.float32)
    if pieces:
        entries = entries * steps_of(stream_key, dims, pieces, -0.22, 0.18)
    return jnp.clip(entries, -most, most).astype(kind)


def setup_inputs(seed: int = 0) -> dict:
    streams_of = jax.random.split(jax.random.key(seed), 5)
    queries = draw_queries(jax.random.fold_in(streams_of[4], 71), 0)
    keys = draw_keys(jax.random.fold_in(streams_of[4], 71), 0)
    values = bell_draw(streams_of[2], (SEQ, GROUPS * HEAD_DIM), 1.0, 6.0, ((0, 32),))
    doc_lengths = ragged(streams_of[3], DOCS, SEQ, SEQ // 4, 1).astype(jnp.int32)
    return dict(queries=queries, keys=keys, values=values, doc_lengths=doc_lengths)


def doc_of(positions, ends):
    return jnp.sum((positions[:, None] >= ends[None, :]).astype(jnp.int32), axis=1)


def reference(queries, keys, values, doc_lengths):
    seq = queries.shape[0]
    per_group = HEADS // GROUPS
    block = TOK_DEV * N_INNER
    span = (OUTER_STEPS + 1) * block
    margin = OUTER_STEPS * block
    scale = HEAD_DIM ** -0.5
    ends = jnp.cumsum(doc_lengths).astype(jnp.int32)
    key_pad = jnp.concatenate([jnp.zeros((margin, GROUPS * HEAD_DIM), keys.dtype), keys], 0)
    value_pad = jnp.concatenate([jnp.zeros((margin, GROUPS * HEAD_DIM), values.dtype), values], 0)
    query_blocks = queries.reshape(seq // TOK_DEV, TOK_DEV, GROUPS, per_group, HEAD_DIM)

    def one_block(index):
        query_rows = query_blocks[index].astype(jnp.float32)
        qpos = (index * TOK_DEV + jnp.arange(TOK_DEV, dtype=jnp.int32)).astype(jnp.int32)
        first = ((index // N_INNER) - OUTER_STEPS) * block
        first = first.astype(jnp.int32)
        key_rows = lax.dynamic_slice_in_dim(key_pad, (first + margin).astype(jnp.int32), span, 0).astype(jnp.float32).reshape(span, GROUPS, HEAD_DIM)
        value_rows = lax.dynamic_slice_in_dim(value_pad, (first + margin).astype(jnp.int32), span, 0).astype(jnp.float32).reshape(span, GROUPS, HEAD_DIM)
        kpos = (first + jnp.arange(span, dtype=jnp.int32)).astype(jnp.int32)
        allowed = (kpos[None, :] <= qpos[:, None]) & (kpos[None, :] >= 0) & (doc_of(kpos, ends)[None, :] == doc_of(qpos, ends)[:, None])
        scores = jnp.einsum("qghd,kgd->qghk", query_rows, key_rows) * scale
        scores = jnp.where(allowed[:, None, None, :], scores, jnp.float32(-1e30))
        top = jnp.max(scores, axis=3, keepdims=True)
        weights = jnp.where(allowed[:, None, None, :], jnp.exp(scores - top), jnp.float32(0.0))
        total = jnp.sum(weights, axis=3)
        rounded = weights.astype(jnp.bfloat16).astype(jnp.float32)
        mixed = jnp.einsum("qghk,kgd->qghd", rounded, value_rows)
        result = mixed / total[:, :, :, None]
        return result.astype(jnp.bfloat16).reshape(TOK_DEV, HEADS * HEAD_DIM)

    outputs = lax.map(one_block, jnp.arange(seq // TOK_DEV, dtype=jnp.int32))
    return outputs.reshape(seq, HEADS * HEAD_DIM)
```

```python
import functools

import jax
import jax.numpy as jnp
from jax import lax
from jax.experimental import pallas as pl
from jax.experimental.pallas import tpu as pltpu
from jax.sharding import PartitionSpec as P

HEADS = 32
GROUPS = 4
HEAD_DIM = 128
OUTER_STEPS = 2
PER_GROUP = HEADS // GROUPS
LOG2E = 1.4426950408889634

NEGATIVE = -1e30

AXES = ("outer", "inner")


def longest_document(seq):
    return seq // 4


def from_behind(array, axis, by):
    size = lax.axis_size(axis)
    pairs = [(i, i + by) for i in range(size) if 0 <= i + by < size]
    return lax.ppermute(array, axis, pairs)


def doc_of(positions, ends):
    return jnp.sum((positions[:, None] >= ends[None, :]).astype(jnp.int32), axis=1)


def tile_update(state, query4, key_rows, value_rows, allowed, scale):
    acc, top, total = state
    scores = (
        jnp.einsum("qghd,kgd->qghk", query4, key_rows, preferred_element_type=jnp.float32) * scale
    )
    scores = jnp.where(allowed[:, None, None, :], scores, NEGATIVE)
    new_top = jnp.maximum(top, jnp.max(scores, axis=3))
    weights = jnp.where(allowed[:, None, None, :], jnp.exp(scores - new_top[:, :, :, None]), 0.0)
    fade = jnp.exp(top - new_top)
    total = total * fade + jnp.sum(weights, axis=3)
    mixed = jnp.einsum(
        "qghk,kgd->qghd",
        weights.astype(jnp.bfloat16),
        value_rows,
        preferred_element_type=jnp.float32,
    )
    acc = acc * fade[:, :, :, None] + mixed
    return (acc, new_top, total)


def attend_tile(state, query4, qpos, qdoc, key_rows, value_rows, kpos, ends, scale):
    kdoc = doc_of(kpos, ends)
    allowed = (
        (kpos[None, :] <= qpos[:, None]) & (kpos[None, :] >= 0) & (kdoc[None, :] == qdoc[:, None])
    )
    return tile_update(state, query4, key_rows, value_rows, allowed, scale)


def attend_rows(state, query4, qpos, qdoc, key_rows, value_rows, kpos, ends, scale):
    count = key_rows.shape[0]
    width = 512
    key_tiles = key_rows.reshape(count // width, width, GROUPS, HEAD_DIM)
    value_tiles = value_rows.reshape(count // width, width, GROUPS, HEAD_DIM)
    pos_tiles = kpos.reshape(count // width, width)

    def visit(carry, item):
        return (
            attend_tile(carry, query4, qpos, qdoc, item[0], item[1], item[2], ends, scale),
            None,
        )

    state, _ = lax.scan(visit, state, (key_tiles, value_tiles, pos_tiles))
    return state


def gathered_body(queries, keys, values, doc_lengths):
    tokens = queries.shape[0]
    scale = HEAD_DIM ** (-0.5)
    n_inner = lax.axis_size("inner")
    outer_index = lax.axis_index("outer")
    inner_index = lax.axis_index("inner")
    block = tokens * n_inner
    ends = jnp.cumsum(doc_lengths)
    query4 = queries.reshape(tokens, GROUPS, PER_GROUP, HEAD_DIM)
    qpos = outer_index * block + inner_index * tokens + jnp.arange(tokens, dtype=jnp.int32)
    qdoc = doc_of(qpos, ends)
    fresh = (
        jnp.zeros((tokens, GROUPS, PER_GROUP, HEAD_DIM), jnp.float32),
        jnp.full((tokens, GROUPS, PER_GROUP), NEGATIVE, jnp.float32),
        jnp.zeros((tokens, GROUPS, PER_GROUP), jnp.float32),
    )
    key_list = [keys]
    value_list = [values]
    for step in range(1, OUTER_STEPS + 1):
        far_pair = from_behind((keys, values), "outer", step)
        key_list.append(far_pair[0])
        value_list.append(far_pair[1])
    stack_keys = jnp.concatenate(key_list, 0)
    stack_values = jnp.concatenate(value_list, 0)
    window = (OUTER_STEPS + 1) * tokens
    piece = (
        lax.all_gather(stack_keys, "inner", axis=0, tiled=True),
        lax.all_gather(stack_values, "inner", axis=0, tiled=True),
    )
    rows = jnp.arange(piece[0].shape[0], dtype=jnp.int32)
    owner = rows // window
    within = rows % window
    kpos = (outer_index - within // tokens) * block + owner * tokens + within % tokens
    state = attend_rows(fresh, query4, qpos, qdoc, piece[0], piece[1], kpos, ends, scale)
    result = state[0] / state[2][:, :, :, None]
    return result.astype(jnp.bfloat16).reshape(tokens, HEADS * HEAD_DIM)


def attend_kernel(tokens, n_inner, slots, first, last, *refs):
    refs = list(refs)
    docs_ref = refs.pop(0) if first else None
    q_ref = refs.pop(0)
    kv_refs = [(refs.pop(0), refs.pop(0)) for _ in slots]
    if not first:
        acc_in, ml_in, rel_in = refs.pop(0), refs.pop(0), refs.pop(0)
    if last:
        out_ref = refs.pop(0)
    else:
        acc_out, ml_out = refs.pop(0), refs.pop(0)
        if first:
            rel_out = refs.pop(0)
    lane = lax.broadcasted_iota(jnp.int32, (tokens, HEAD_DIM), 1)
    if first:
        base = (lax.axis_index("outer") * n_inner + lax.axis_index("inner")) * tokens
        row = lax.broadcasted_iota(jnp.int32, (tokens, HEAD_DIM), 0)
        rel = jnp.full((tokens, HEAD_DIM), -base, jnp.int32)
        end = -base
        for i in range(docs_ref.shape[0]):
            end = end + docs_ref[i]
            rel = jnp.where(row >= end, end, rel)
        rel_out[...] = rel
    else:
        rel = rel_in[...]
    odd = lax.rem(lax.axis_index("inner"), 2)
    bias = []
    for distance, sway in slots:
        start = -tokens * (distance + sway * odd)
        seen = lane + start >= rel
        if distance == 0 and sway == 0:
            seen = seen & (lane <= row)
        bias.append(jnp.where(seen, 0.0, NEGATIVE).astype(jnp.float32))
    bias = jnp.concatenate(bias, axis=1)
    key_rows = jnp.concatenate([k[...] for k, _ in kv_refs], axis=0)
    value_rows = jnp.concatenate([v[...] for _, v in kv_refs], axis=0)
    factor = HEAD_DIM ** (-0.5) * LOG2E
    ml = jnp.zeros((tokens, HEAD_DIM), jnp.float32)
    for h in range(PER_GROUP):
        cols = slice(h * HEAD_DIM, (h + 1) * HEAD_DIM)
        scores = lax.dot_general(
            q_ref[:, cols], key_rows, (((1,), (1,)), ((), ())), preferred_element_type=jnp.float32
        )
        scores = scores + bias
        top = jnp.max(scores, axis=1, keepdims=True)
        if not first:
            old_top = ml_in[0, :, h : h + 1]
            top = jnp.maximum(top, old_top)
            fade = jnp.exp2((old_top - top) * factor)
        weights = jnp.exp2((scores - top) * factor)
        total = jnp.sum(weights, axis=1, keepdims=True)
        mixed = lax.dot_general(
            weights.astype(jnp.bfloat16),
            value_rows,
            (((1,), (0,)), ((), ())),
            preferred_element_type=jnp.float32,
        )
        if not first:
            total = total + ml_in[0, :, PER_GROUP + h : PER_GROUP + h + 1] * fade
            mixed = mixed + acc_in[:, cols] * fade
        if last:
            out_ref[:, cols] = (mixed / total).astype(out_ref.dtype)
        else:
            acc_out[:, cols] = mixed
            ml = jnp.where(lane == h, top, ml)
            ml = jnp.where(lane == PER_GROUP + h, total, ml)
    if not last:
        ml_out[0] = ml


def attend(queries, docs, slots, state, last, n_inner):
    tokens = queries.shape[0]
    first = state is None
    wide = PER_GROUP * HEAD_DIM
    wide_spec = pl.BlockSpec((tokens, wide), lambda g: (0, g))
    ml_spec = pl.BlockSpec((1, tokens, HEAD_DIM), lambda g: (g, 0, 0))
    rel_spec = pl.BlockSpec((tokens, HEAD_DIM), lambda g: (0, 0))
    args, specs = [], []
    if first:
        args.append(docs)
        specs.append(pl.BlockSpec(memory_space=pltpu.SMEM))
    args.append(queries)
    specs.append(wide_spec)
    for (k, v), _, _ in slots:
        if k is v:
            args += [k, k]
            specs.append(pl.BlockSpec((tokens, HEAD_DIM), lambda g: (0, g)))
            specs.append(pl.BlockSpec((tokens, HEAD_DIM), lambda g: (0, g + GROUPS)))
        else:
            args += [k, v]
            specs += [pl.BlockSpec((tokens, HEAD_DIM), lambda g: (0, g))] * 2
    if not first:
        args += list(state)
        specs += [wide_spec, ml_spec, rel_spec]
    if last:
        out_shape = jax.ShapeDtypeStruct((tokens, HEADS * HEAD_DIM), jnp.bfloat16)
        out_specs = wide_spec
    else:
        out_shape = [
            jax.ShapeDtypeStruct((tokens, HEADS * HEAD_DIM), jnp.float32),
            jax.ShapeDtypeStruct((GROUPS, tokens, HEAD_DIM), jnp.float32),
        ]
        out_specs = [wide_spec, ml_spec]
        if first:
            out_shape.append(jax.ShapeDtypeStruct((tokens, HEAD_DIM), jnp.int32))
            out_specs.append(rel_spec)
    keys_seen = len(slots) * tokens
    result = pl.pallas_call(
        functools.partial(
            attend_kernel, tokens, n_inner, tuple((d, s) for _, d, s in slots), first, last
        ),
        grid=(GROUPS,),
        in_specs=specs,
        out_specs=out_specs,
        out_shape=out_shape,
        cost_estimate=pl.CostEstimate(
            flops=4 * HEADS * HEAD_DIM * tokens * keys_seen,
            bytes_accessed=tokens * HEADS * HEAD_DIM * 8,
            transcendentals=HEADS * tokens * keys_seen,
        ),
        compiler_params=pltpu.CompilerParams(
            dimension_semantics=("arbitrary",), vmem_limit_bytes=24 * 1024 * 1024
        ),
    )(*args)
    if last:
        return result
    return (result[0], result[1], state[2] if not first else result[2])


def window_body(reach, queries, keys, values, doc_lengths):
    n_inner = lax.axis_size("inner")
    shards = lax.axis_size("outer") * n_inner
    half = reach // 2

    def move(array, pairs):
        return lax.ppermute(array, AXES, pairs)

    def behind(array, by):
        return move(array, [(s, s + 2 * by) for s in range(shards - 2 * by)])

    swap = [(s, s ^ 1) for s in range(shards)]
    own = jnp.concatenate([keys, values], axis=1)
    near = {1: behind(own, 1)}
    side = {0: move(own, swap)}
    for k in range(3, half):
        near[k] = behind(own, k)
    near[half] = behind(own, half)
    side[1] = move(near[1], swap)
    if half > 2:
        near[2] = behind(near[1], 1)
    for k in range(3, half):
        side[k] = move(near[k], swap)
    far = move(side[0], [(s, s + 2 * half) for s in range(shards - 2 * half) if s % 2 == 0])
    if half > 2:
        side[2] = move(near[2], swap)
    odd = lax.axis_index("inner") % 2 == 1
    edge = jnp.where(odd, side[0], far)

    def slot_near(k):
        return ((near[k], near[k]), 2 * k, 0)

    def slot_side(k):
        return ((side[k], side[k]), 2 * k - 1, 2)

    early = [((keys, values), 0, 0), slot_near(1)]
    middle = [((edge, edge), 2 * half - 1, 2 - 2 * half)]
    middle += [slot_side(1)]
    for k in range(3, half):
        middle += [slot_near(k), slot_side(k)]
    middle += [slot_near(half)]
    if half > 2:
        middle += [slot_near(2)]
    state = attend(queries, doc_lengths, early, None, False, n_inner)
    if half > 2:
        state = attend(queries, None, middle, state, False, n_inner)
        return attend(queries, None, [slot_side(2)], state, True, n_inner)
    return attend(queries, None, middle, state, True, n_inner)


def solution(mesh):
    in_specs = (P(AXES, None), P(AXES, None), P(AXES, None), P())
    out_specs = P(AXES, None)
    shards = mesh.shape["outer"] * mesh.shape["inner"]

    def run(queries, keys, values, doc_lengths):
        seq = queries.shape[0]
        tokens = seq // shards
        reach = -(-(longest_document(seq) - 1) // tokens)
        short = reach <= mesh.shape["inner"] and reach % 2 == 0 and mesh.shape["inner"] % 2 == 0
        body = functools.partial(window_body, reach) if short else gathered_body
        return jax.shard_map(
            body, mesh=mesh, in_specs=in_specs, out_specs=out_specs, check_vma=False
        )(queries, keys, values, doc_lengths)

    return run
```
